256 devices in a mesh: station: 4 (over x, y), tm: 64 (over z, core).
Axes of the slice: x: 2, y: 2, z: 32, core: 2. Of those that a mesh axis runs over, the one named last changes fastest.
The devices are a block of a 4x8x32 slice.
Arguments:
- spectra: float32 [512, 8, 16384], P('tm', 'station'), parts along dimension 1, may hold values from -6 to 6
- synth_taps: float32 [16, 512], replicated, may hold values from -1.5 to 1.5
- analysis_taps: float32 [16, 512], replicated, may hold values from -1.5 to 1.5
Outputs:
- channels: float32 [512, 8, 20480], P('tm', 'station'), parts along dimension 1
The draws below stay inside these ranges and needn't reach their ends.
There are 4 independent parts, one for each index of `station`. The reference program is written for one: setup_inputs(seed, part) draws one part's arguments, and reference() takes and returns one part's arrays. A program takes and returns all parts, laid end to end along the dimension named above; an argument that names none is the same for every part. Nothing has to cross between parts.
All inputs are finite; a program needn't handle non-finite values.
Results may differ from the reference program's by a relative error of at most 0.00007.
Values sent between devices are 32-bit elements; how exact they have to be, the bound alone decides.
A program may use at most 64 MiB of HBM per device.

```python
import math
import jax
import jax.numpy as jnp
from jax import lax

M = 512
P_SIZE = 16
RT = 32
PHASES = 64
FRAMES = 16384


def block_scale(own_key, extent, shards, low, top_value):
    def one(dim, shards_of):
        heights = jax.random.uniform(jax.random.fold_in(jax.random.fold_in(own_key, 6), dim), (shards_of,), jnp.float32, low / len(shards), top_value / len(shards))
        return jnp.repeat(jnp.exp(heights), extent[dim] // shards_of).reshape((-1,) + (1,) * (len(extent) - dim - 1))

    factor_of = one(*shards[0])
    for cut in shards[1:]:
        factor_of = factor_of * one(*cut)
    return factor_of


def noise(own_key, extent, scale, reach, shards=(), kind=jnp.bfloat16):
    values = scale * jax.random.normal(own_key, extent, jnp.float32)
    if shards:
        values = values * block_scale(own_key, extent, shards, -0.22, 0.18)
    return jnp.clip(values, -reach, reach).astype(kind)


def setup_inputs(seed: int = 0, part: int = 0) -> dict:
    arg_keys = jax.random.split(jax.random.key(seed), 4)
    part_splits = jax.random.split(jax.random.fold_in(arg_keys[3], part), 4)
    spectra = noise(part_splits[0], (M, 2, FRAMES), 1.0, 6.0, ((0, 64),), jnp.float32)
    synth_taps = noise(arg_keys[1], (P_SIZE, M), P_SIZE ** -0.5, 1.5, (), jnp.float32)
    analysis_taps = noise(arg_keys[2], (P_SIZE, M), P_SIZE ** -0.5, 1.5, (), jnp.float32)
    return {"spectra": spectra, "synth_taps": synth_taps, "analysis_taps": analysis_taps}


def tables(width):
    index = jnp.arange(width, dtype=jnp.int32)
    product = index[:, None] * index[None, :] % width
    angle = product.astype(jnp.float32) * (2.0 * math.pi / width)
    scale = 1.0 / math.sqrt(width)
    return (jnp.cos(angle) * scale, jnp.sin(angle) * scale)

def resampler(width, taps_len, phases):
    out_width = 5 * width // 4
    sample = jnp.arange(out_width, dtype=jnp.int32)[:, None]
    column = jnp.arange(2 * width, dtype=jnp.int32)[None, :]
    start = 4 * sample // 5
    phase = phases * (4 * sample % 5) // 5
    lag = start + width - column
    offset = lag.astype(jnp.float32) + phase.astype(jnp.float32) / phases - (taps_len // 2 - 1)
    window = 0.5 + 0.5 * jnp.cos(math.pi * offset / (taps_len / 2.0))
    coeff = 0.9 * jnp.sinc(0.9 * offset) * window
    valid = (lag >= 0) & (lag < taps_len)
    full = jnp.where(valid, coeff, jnp.zeros_like(coeff))
    return (full[:, width:], full[:, :width])

def inverse(raw, cosines, sines):
    dims = (((0,), (0,)), ((), ()))
    with_cos = lax.dot_general(raw, cosines, dims, precision=lax.Precision.HIGHEST, preferred_element_type=jnp.float32)
    with_sin = lax.dot_general(raw, sines, dims, precision=lax.Precision.HIGHEST, preferred_element_type=jnp.float32)
    return jnp.stack([with_cos[0] - with_sin[1], with_sin[0] + with_cos[1]])

def forward(frames, cosines, sines):
    dims = (((1,), (2,)), ((), ()))
    with_cos = lax.dot_general(cosines, frames, dims, precision=lax.Precision.HIGHEST, preferred_element_type=jnp.float32)
    with_sin = lax.dot_general(sines, frames, dims, precision=lax.Precision.HIGHEST, preferred_element_type=jnp.float32)
    return jnp.stack([with_cos[:, 0] + with_sin[:, 1], with_cos[:, 1] - with_sin[:, 0]], axis=1)

def filtered(frames, taps):
    count = frames.shape[1] - taps.shape[0] + 1
    total = jnp.zeros((2, count, frames.shape[2]), frames.dtype)
    for lag_index in range(taps.shape[0]):
        first = taps.shape[0] - 1 - lag_index
        total = total + taps[lag_index][None, None, :] * frames[:, first:first + count]
    return total

def resample(stream, current, previous):
    width = stream.shape[2]
    now_rows = stream[:, 1:].reshape(-1, width)
    before_rows = stream[:, :-1].reshape(-1, width)
    dims = (((1,), (1,)), ((), ()))
    out = lax.dot_general(now_rows, current, dims, precision=lax.Precision.HIGHEST, preferred_element_type=jnp.float32)
    out = out + lax.dot_general(before_rows, previous, dims, precision=lax.Precision.HIGHEST, preferred_element_type=jnp.float32)
    return out.reshape(2, -1, width)

def reference(spectra, synth_taps, analysis_taps):
    cosines, sines = tables(M)
    current, previous = resampler(M, RT, PHASES)
    spread = inverse(spectra, cosines, sines)
    padded = jnp.concatenate([jnp.zeros((2, P_SIZE - 1, M), spread.dtype), spread], axis=1)
    stream = filtered(padded, synth_taps)
    stream = jnp.concatenate([jnp.zeros((2, 1, M), stream.dtype), stream], axis=1)
    resampled = resample(stream, current, previous)
    resampled = jnp.concatenate([jnp.zeros((2, P_SIZE - 1, M), resampled.dtype), resampled], axis=1)
    windowed = filtered(resampled, analysis_taps)
    return forward(windowed, cosines, sines)
```

```python
import functools
import math

import jax
import jax.numpy as jnp
import numpy as np
from jax import lax
from jax.experimental import pallas as pl
from jax.experimental.pallas import tpu as pltpu
from jax.sharding import PartitionSpec as P

RT = 32
PHASES = 64
UP, DOWN = 5, 4
W = 64
L = 128
HALO = 32
BACK = 16
MESH = pl.DeviceIdType.MESH
F32 = jnp.float32


def split(a):
    hi = a.astype(jnp.bfloat16)
    return hi, (a - hi.astype(F32)).astype(jnp.bfloat16)


def dft_table(width):
    k = np.outer(np.arange(width), np.arange(width)) % width
    angle = k * (2.0 * math.pi / width)
    both = np.concatenate([np.cos(angle), np.sin(angle)], axis=1) / math.sqrt(width)
    return both.astype(np.float32)


def resample_table(width):
    out_width = UP * width // DOWN
    sample = np.arange(out_width)[None, :]
    row = np.arange(L + width)[:, None]
    lag = DOWN * sample // UP + L - row
    phase = PHASES * (DOWN * sample % UP) // UP
    t = lag + phase / PHASES - (RT // 2 - 1)
    coeff = 0.9 * np.sinc(0.9 * t) * (0.5 + 0.5 * np.cos(math.pi * t / (RT / 2.0)))
    return np.where((lag >= 0) & (lag < RT), coeff, 0.0).astype(np.float32)


def halves(table):
    hi = table.astype(jnp.bfloat16)
    lo = (table - hi.astype(np.float32)).astype(jnp.bfloat16)
    return jnp.asarray(np.stack([hi, lo]))


def product(a, b, dims):
    (ah, al), (bh, bl) = a, b
    dot = lambda x, y: lax.dot_general(x, y, (dims, ((), ())), preferred_element_type=F32)
    return dot(ah, bh) + (dot(ah, bl) + dot(al, bh))


def kernel(
    n, x_ref, st_ref, at_ref, cs_hbm, rs_hbm, o_ref,
    cs, rs, xs, land1, v_all, hbuf, vwin, ywin, zst, zfull, zwin, u2, sbuf, land2,
    csem, rsem, send1, recv1, hsend, hrecv, send2, recv2,
):
    me = lax.axis_index("tm")
    station = lax.axis_index("station")
    nc = n // 2
    chip, core = me // 2, me % 2
    taps = st_ref.shape[0]
    m = st_ref.shape[1]
    chunks = land1.shape[0]
    pieces = land2.shape[0]
    cb = x_ref.shape[1]
    blocks = m // L

    barrier = pltpu.get_barrier_semaphore()

    def greet(j, c):
        pl.semaphore_signal(barrier, inc=1, device_id=(station, (me + j) % n), device_id_type=MESH)
        return c

    lax.fori_loop(1, n, greet, 0)
    get_cs = pltpu.make_async_copy(cs_hbm, cs, csem)
    get_rs = pltpu.make_async_copy(rs_hbm, rs, rsem)
    get_cs.start()
    get_rs.start()

    low = lax.broadcasted_iota(jnp.int32, (cb, L), 1) < W

    def arrange(t, c):
        a = x_ref[0, :, pl.ds(pl.multiple_of(t * L, L), L)]
        b = x_ref[1, :, pl.ds(pl.multiple_of(t * L, L), L)]
        xs[2 * t] = jnp.where(low, a, pltpu.roll(b, W, 1))
        xs[2 * t + 1] = jnp.where(low, pltpu.roll(a, W, 1), b)
        return c

    lax.fori_loop(0, n * chunks // 2, arrange, 0)
    ywin[:, 0:8, :] = jnp.zeros((2, 8, m), F32)
    pl.semaphore_wait(barrier, n - 1)

    def send_to_all(source, target, sent, got):
        def send(dev):
            pltpu.make_async_remote_copy(
                src_ref=source(dev), dst_ref=target, send_sem=sent, recv_sem=got,
                device_id=(station, dev), device_id_type=MESH,
            ).start()

        def step(j, c):
            jj = j // 2
            d = nc // 2 - jj // 2
            sign = 1 - 2 * (jj % 2)
            dev = ((chip + sign * d + nc) % nc) * 2 + (j % 2 + core) % 2

            @pl.when(jnp.logical_not(jnp.logical_and(2 * d == nc, sign == -1)))
            def _():
                send(dev)

            return c

        lax.fori_loop(0, 2 * nc, step, 0)
        send(chip * 2 + 1 - core)

    def wait_bytes(ref, sem):
        part = ref.at[pl.ds(0, n - 1)]
        pltpu.make_async_copy(part, part, sem).wait()

    def send_in(k):
        send_to_all(lambda dev: xs.at[dev * chunks + k], land1.at[k, me], send1.at[k], recv1.at[k])
        land1[k, me] = xs[me * chunks + k]

    def synthesize(k):
        wait_bytes(land1.at[k], recv1.at[k])
        raw = land1[k].reshape(m, L)
        out = product(split(raw.T), (cs[0], cs[1]), ((1,), (0,)))
        v_all[k, 0] = out[:W, :m] - out[W:, m:]
        v_all[k, 1] = out[:W, m:] + out[W:, :m]

    last = chunks - 1
    send_in(last)
    send_in(0)
    get_cs.wait()
    synthesize(last)
    tail = pltpu.make_async_remote_copy(
        src_ref=v_all.at[last, :, pl.ds(W - HALO, HALO)], dst_ref=hbuf,
        send_sem=hsend, recv_sem=hrecv,
        device_id=(station, (me + 1) % n), device_id_type=MESH,
    )

    @pl.when(me < n - 1)
    def _():
        tail.start()

    def send_rest(k, c):
        send_in(k)
        return c

    lax.fori_loop(1, last, send_rest, 0)
    get_rs.wait()

    def resampled(k):
        @pl.when(k == 0)
        def _():
            @pl.when(me == 0)
            def _():
                vwin[:, 0:HALO, :] = jnp.zeros((2, HALO, m), F32)

            @pl.when(me > 0)
            def _():
                tail.wait_recv()
                vwin[:, 0:HALO, :] = hbuf[...]

        @pl.when(k > 0)
        def _():
            vwin[:, 0:HALO, :] = vwin[:, W : W + HALO, :]

        vwin[:, HALO:, :] = v_all[k]
        rows = BACK + W
        for ri in range(2):
            for b in range(blocks):
                lanes = pl.ds(b * L, L)
                total = jnp.zeros((rows, L), F32)
                for p in range(taps):
                    total = total + st_ref[p : p + 1, lanes] * vwin[ri, pl.ds(BACK - p, rows), lanes]
                ywin[ri, pl.ds(8, rows), lanes] = total
        left = jnp.concatenate(
            [
                jnp.concatenate([ywin[ri, pl.ds(7, rows), pl.ds(m - L, L)], ywin[ri, pl.ds(8, rows), :]], axis=1)
                for ri in range(2)
            ],
            axis=0,
        )
        out = product(split(left), (rs[0], rs[1]), ((1,), (0,)))
        wide = UP * blocks // DOWN
        for ri in range(2):
            for j in range(wide):
                zst[ri, pl.ds(j, rows, stride=wide), :] = out[ri * rows : (ri + 1) * rows, j * L : (j + 1) * L]

        @pl.when(k == 0)
        def _():
            zfull[:, 0 : BACK * wide, :] = zst[:, 0 : BACK * wide, :]

        zfull[:, pl.ds(pl.multiple_of(BACK * wide + k * (W * wide), 8), W * wide), :] = zst[:, BACK * wide :, :]

    def analyzed(p):
        wide = UP * blocks // DOWN
        first = BACK * wide - BACK * blocks
        zwin[...] = zfull[:, pl.ds(pl.multiple_of(first + p * (W * blocks), 8), (BACK + W) * blocks), :]
        for b in range(blocks):
            for ri in range(2):
                total = jnp.zeros((W, L), F32)
                for t in range(taps):
                    total = total + at_ref[t : t + 1, pl.ds(b * L, L)] * zwin[
                        ri, pl.ds((BACK - t) * blocks + b, W, stride=blocks), :
                    ]
                if ri == 0:
                    u2[0:W, pl.ds(b * L, L)] = total
                    u2[W:, pl.ds(m + b * L, L)] = -total
                else:
                    u2[0:W, pl.ds(m + b * L, L)] = total
                    u2[W:, pl.ds(b * L, L)] = total
        out = product((cs[0], cs[1]), split(u2[...]), ((1,), (1,)))
        sbuf[p] = out.reshape(n, cb, L)
        land2[p, me] = sbuf[p, me]
        send_to_all(lambda dev: sbuf.at[p, dev], land2.at[p, me], send2.at[p], recv2.at[p])

    def step(p, c):
        @pl.when(p < last)
        def _():
            synthesize(p)

        @pl.when(p < chunks)
        def _():
            resampled(p)

        analyzed(p)
        return c

    lax.fori_loop(0, pieces, step, 0)

    @pl.when(me < n - 1)
    def _():
        tail.wait_send()

    for k in range(chunks):
        wait_bytes(land1.at[k], send1.at[k])
    for p in range(pieces):
        wait_bytes(land2.at[p], recv2.at[p])

    def place(t, c):
        for u in range(pieces):
            a = land2[(2 * u) % pieces, 2 * t + (2 * u) // pieces]
            b = land2[(2 * u + 1) % pieces, 2 * t + (2 * u + 1) // pieces]
            lanes = pl.ds(pl.multiple_of(t * (pieces * L) + u * L, L), L)
            o_ref[0, :, lanes] = jnp.where(low, a, pltpu.roll(b, W, 1))
            o_ref[1, :, lanes] = jnp.where(low, pltpu.roll(a, W, 1), b)
        return c

    lax.fori_loop(0, n // 2, place, 0)
    for p in range(pieces):
        wait_bytes(land2.at[p], send2.at[p])


def shards(n, spectra, synth_taps, analysis_taps):
    cb, _, frames = spectra.shape
    m = synth_taps.shape[1]
    own = frames // n
    chunks = own // W
    pieces = UP * own // DOWN // W
    wide = UP * m // DOWN // L
    blocks = m // L
    vmem = pl.BlockSpec(memory_space=pltpu.VMEM)
    hbm = pl.BlockSpec(memory_space=pl.ANY)
    dma = pltpu.SemaphoreType.DMA
    out = pl.pallas_call(
        functools.partial(kernel, n),
        out_shape=jax.ShapeDtypeStruct((2, cb, UP * frames // DOWN), F32),
        in_specs=[vmem, vmem, vmem, hbm, hbm],
        out_specs=vmem,
        scratch_shapes=[
            pltpu.VMEM((2, m, 2 * m), jnp.bfloat16),
            pltpu.VMEM((2, m + L, wide * L), jnp.bfloat16),
            pltpu.VMEM((n * chunks, cb, L), F32),
            pltpu.VMEM((chunks, n, cb, L), F32),
            pltpu.VMEM((chunks, 2, W, m), F32),
            pltpu.VMEM((2, HALO, m), F32),
            pltpu.VMEM((2, HALO + W, m), F32),
            pltpu.VMEM((2, 8 + BACK + W, m), F32),
            pltpu.VMEM((2, (BACK + W) * wide, L), F32),
            pltpu.VMEM((2, (BACK + own) * wide, L), F32),
            pltpu.VMEM((2, (BACK + W) * blocks, L), F32),
            pltpu.VMEM((2 * W, 2 * m), F32),
            pltpu.VMEM((pieces, n, cb, L), F32),
            pltpu.VMEM((pieces, n, cb, L), F32),
            dma, dma, dma((chunks,)), dma((chunks,)), dma, dma, dma((pieces,)), dma((pieces,)),
        ],
        compiler_params=pltpu.CompilerParams(
            collective_id=0, has_side_effects=True, vmem_limit_bytes=40 << 20
        ),
    )(
        jnp.swapaxes(spectra, 0, 1), synth_taps, analysis_taps,
        halves(dft_table(m)), halves(resample_table(m)),
    )
    return jnp.swapaxes(out, 0, 1)


def solution(mesh):
    in_specs = (P("tm", "station", None), P(), P())
    out_specs = P("tm", "station", None)
    body = functools.partial(shards, mesh.shape["tm"])
    return jax.shard_map(body, mesh=mesh, in_specs=in_specs, out_specs=out_specs, check_vma=False)
```

```python
import functools
import math

import jax
import jax.numpy as jnp
import numpy as np
from jax import lax
from jax.experimental import pallas as pl
from jax.experimental.pallas import tpu as pltpu
from jax.sharding import PartitionSpec as P

RT = 32
PHASES = 64
UP, DOWN = 5, 4
REACH = 4
W = 64
L = 128
HALO = 32
BACK = 16
MESH = pl.DeviceIdType.MESH
F32 = jnp.float32


def split(a):
    hi = a.astype(jnp.bfloat16)
    return hi, (a - hi.astype(F32)).astype(jnp.bfloat16)


def dft_table(width):
    k = np.outer(np.arange(width), np.arange(width)) % width
    angle = k * (2.0 * math.pi / width)
    both = np.concatenate([np.cos(angle), np.sin(angle)], axis=1) / math.sqrt(width)
    return both.astype(np.float32)


def resample_table(width):
    out_width = UP * width // DOWN
    sample = np.arange(out_width)[None, :]
    row = np.arange(L + width)[:, None]
    lag = DOWN * sample // UP + L - row
    phase = PHASES * (DOWN * sample % UP) // UP
    t = lag + phase / PHASES - (RT // 2 - 1)
    coeff = 0.9 * np.sinc(0.9 * t) * (0.5 + 0.5 * np.cos(math.pi * t / (RT / 2.0)))
    return np.where((lag >= 0) & (lag < RT), coeff, 0.0).astype(np.float32)


def halves(table):
    hi = table.astype(jnp.bfloat16)
    lo = (table - hi.astype(np.float32)).astype(jnp.bfloat16)
    return jnp.asarray(np.stack([hi, lo]))


def product(a, b, dims):
    (ah, al), (bh, bl) = a, b
    dot = lambda x, y: lax.dot_general(x, y, (dims, ((), ())), preferred_element_type=F32)
    return dot(ah, bh) + (dot(ah, bl) + dot(al, bh))


def kernel(
    n, x_hbm, st_hbm, at_hbm, cs_hbm, rs_hbm, o_ref,
    x_ref, st_ref, at_ref, cs, rs, xs, land1, v_all, hbuf, vwin, ywin, zst, zfull, zwin, u2, sbuf, land2,
    xsem, ssem, asem, csem, rsem, send1, recv1, hsend, hrecv, send2, recv2, ready,
):
    me = lax.axis_index("tm")
    station = lax.axis_index("station")
    nc = n // 2
    chip, core = me // 2, me % 2
    taps = st_ref.shape[0]
    m = st_ref.shape[1]
    chunks = land1.shape[0]
    pieces = land2.shape[0]
    cb = xs.shape[1]
    out_rows = o_ref.shape[0] // cb
    blocks = m // L

    def at(offset, c):
        return (chip + offset + nc) % nc * 2 + c

    def signal(sem, dev):
        pl.semaphore_signal(sem, inc=1, device_id=(station, dev), device_id_type=MESH)

    barrier = pltpu.get_barrier_semaphore()
    half = nc // 2
    reach = min(REACH, half)
    met = 1
    signal(barrier, at(0, 1 - core))
    for d in range(1, reach + 1):
        for offset in (d,) if 2 * d == nc else (d, -d):
            for c in range(2):
                signal(barrier, at(offset, c))
                met += 1
    in_rows = x_hbm.shape[0] // cb
    pitch = x_ref.shape[0] // cb
    get_x = [
        pltpu.make_async_copy(
            x_hbm.at[pl.ds(i * in_rows, in_rows)], x_ref.at[pl.ds(i * pitch, in_rows)], xsem.at[i]
        )
        for i in range(cb)
    ]
    for copy in get_x:
        copy.start()
    get_cs = pltpu.make_async_copy(cs_hbm, cs, csem)
    get_rs = pltpu.make_async_copy(rs_hbm, rs, rsem)
    get_st = pltpu.make_async_copy(st_hbm, st_ref, ssem)
    get_at = pltpu.make_async_copy(at_hbm, at_ref, asem)
    for copy in (get_cs, get_rs, get_st, get_at):
        copy.start()

    low = lax.broadcasted_iota(jnp.int32, (cb, L), 1) < W

    def arrange(i, c):
        for t in [chunks * i + j for j in range(chunks)]:
            a = x_ref[pl.ds(2 * t, cb, stride=pitch), :]
            b = x_ref[pl.ds(2 * t + 1, cb, stride=pitch), :]
            xs[2 * t] = jnp.where(low, a, pltpu.roll(b, W, 1))
            xs[2 * t + 1] = jnp.where(low, pltpu.roll(a, W, 1), b)
        return c

    def send_to(source, target, sent, got, near, far):
        def send(dev):
            pltpu.make_async_remote_copy(
                src_ref=source(dev), dst_ref=target, send_sem=sent, recv_sem=got,
                device_id=(station, dev), device_id_type=MESH,
            ).start()

        def step(j, c):
            d = far - j // 4
            sign = 1 - 2 * (j // 2 % 2)

            @pl.when(jnp.logical_not(jnp.logical_and(2 * d == nc, sign == -1)))
            def _():
                send(at(sign * d, (j + core) % 2))

            return c

        lax.fori_loop(0, 4 * (far - near + 1), step, 0)
        if near == 1:
            send(at(0, 1 - core))

    def send_in(k, near, far):
        send_to(lambda dev: xs.at[dev * chunks + k], land1.at[k, me], send1.at[k], recv1.at[k], near, far)

    def wait_bytes(ref, sem):
        part = ref.at[pl.ds(0, n - 1)]
        pltpu.make_async_copy(part, part, sem).wait()

    def synthesize(k):
        wait_bytes(land1.at[k], recv1.at[k])
        raw = land1[k].reshape(m, L)
        out = product(split(raw.T), (cs[0], cs[1]), ((1,), (0,)))
        v_all[k, 0] = out[:W, :m] - out[W:, m:]
        v_all[k, 1] = out[:W, m:] + out[W:, :m]

    last = chunks - 1
    for copy in get_x:
        copy.wait()
    lax.fori_loop(0, n // 2, arrange, 0)
    pl.semaphore_wait(barrier, met)
    known, turn, done = reach, 0, 0
    while known < half:
        for offset in (known, -known):
            signal(ready.at[turn], at(offset, core))
        for k in range(chunks):
            send_in((k - 1) % chunks, done + 1, known)
        done = known
        pl.semaphore_wait(ready.at[turn], 2)
        known, turn = min(2 * known, half), turn + 1
    send_in(last, done + 1, half)
    send_in(0, done + 1, half)
    for k in range(chunks):
        land1[k, me] = xs[me * chunks + k]
    ywin[:, 0:8, :] = jnp.zeros((2, 8, m), F32)
    get_cs.wait()
    synthesize(last)
    tail = pltpu.make_async_remote_copy(
        src_ref=v_all.at[last, :, pl.ds(W - HALO, HALO)], dst_ref=hbuf,
        send_sem=hsend, recv_sem=hrecv,
        device_id=(station, (me + 1) % n), device_id_type=MESH,
    )

    @pl.when(me < n - 1)
    def _():
        tail.start()

    for k in range(1, last):
        send_in(k, done + 1, half)
    for copy in (get_rs, get_st, get_at):
        copy.wait()

    def resampled(k):
        @pl.when(k == 0)
        def _():
            @pl.when(me == 0)
            def _():
                vwin[:, 0:HALO, :] = jnp.zeros((2, HALO, m), F32)

            @pl.when(me > 0)
            def _():
                tail.wait_recv()
                vwin[:, 0:HALO, :] = hbuf[...]

        @pl.when(k > 0)
        def _():
            vwin[:, 0:HALO, :] = vwin[:, W : W + HALO, :]

        vwin[:, HALO:, :] = v_all[k]
        rows = BACK + W
        for ri in range(2):
            for b in range(blocks):
                lanes = pl.ds(b * L, L)
                total = jnp.zeros((rows, L), F32)
                for p in range(taps):
                    total = total + st_ref[p : p + 1, lanes] * vwin[ri, pl.ds(BACK - p, rows), lanes]
                ywin[ri, pl.ds(8, rows), lanes] = total
        left = jnp.concatenate(
            [
                jnp.concatenate([ywin[ri, pl.ds(7, rows), pl.ds(m - L, L)], ywin[ri, pl.ds(8, rows), :]], axis=1)
                for ri in range(2)
            ],
            axis=0,
        )
        out = product(split(left), (rs[0], rs[1]), ((1,), (0,)))
        wide = UP * blocks // DOWN
        for ri in range(2):
            for j in range(wide):
                zst[ri, pl.ds(j, rows, stride=wide), :] = out[ri * rows : (ri + 1) * rows, j * L : (j + 1) * L]

        @pl.when(k == 0)
        def _():
            zfull[:, 0 : BACK * wide, :] = zst[:, 0 : BACK * wide, :]

        zfull[:, pl.ds(pl.multiple_of(BACK * wide + k * (W * wide), 8), W * wide), :] = zst[:, BACK * wide :, :]

    def analyzed(p):
        wide = UP * blocks // DOWN
        first = BACK * wide - BACK * blocks
        zwin[...] = zfull[:, pl.ds(pl.multiple_of(first + p * (W * blocks), 8), (BACK + W) * blocks), :]
        for b in range(blocks):
            for ri in range(2):
                total = jnp.zeros((W, L), F32)
                for t in range(taps):
                    total = total + at_ref[t : t + 1, pl.ds(b * L, L)] * zwin[
                        ri, pl.ds((BACK - t) * blocks + b, W, stride=blocks), :
                    ]
                if ri == 0:
                    u2[0:W, pl.ds(b * L, L)] = total
                    u2[W:, pl.ds(m + b * L, L)] = -total
                else:
                    u2[0:W, pl.ds(m + b * L, L)] = total
                    u2[W:, pl.ds(b * L, L)] = total
        out = product((cs[0], cs[1]), split(u2[...]), ((1,), (1,)))
        sbuf[p] = out.reshape(n, cb, L)
        land2[p, me] = sbuf[p, me]
        send_to(lambda dev: sbuf.at[p, dev], land2.at[p, me], send2.at[p], recv2.at[p], 1, nc // 2)

    def step(p, c):
        @pl.when(p < last)
        def _():
            synthesize(p)

        @pl.when(p < chunks)
        def _():
            resampled(p)

        analyzed(p)
        return c

    lax.fori_loop(0, pieces, step, 0)

    @pl.when(me < n - 1)
    def _():
        tail.wait_send()

    for k in range(chunks):
        wait_bytes(land1.at[k], send1.at[k])
    for p in range(pieces):
        wait_bytes(land2.at[p], recv2.at[p])
        pairs = [(u, divmod(2 * u, pieces), divmod(2 * u + 1, pieces)) for u in range(pieces)]
        pairs = [pair for pair in pairs if max(pair[1][1], pair[2][1]) == p]

        def place(t, c, pairs=pairs):
            for u, (da, pa), (db, pb) in pairs:
                a = land2[pa, 2 * t + da]
                b = land2[pb, 2 * t + db]
                first = 2 * (t * pieces + u)
                o_ref[pl.ds(first, cb, stride=out_rows), :] = jnp.where(low, a, pltpu.roll(b, W, 1))
                o_ref[pl.ds(first + 1, cb, stride=out_rows), :] = jnp.where(low, pltpu.roll(a, W, 1), b)
            return c

        if pairs:
            lax.fori_loop(0, n // 2, place, 0)

    for p in range(pieces):
        wait_bytes(land2.at[p], send2.at[p])


def rows_of(spectra):
    parts = spectra.reshape(spectra.shape[0], 2, -1, L)
    return jnp.swapaxes(parts, 1, 2).reshape(-1, L)


def shards(n, spectra, synth_taps, analysis_taps):
    cb, _, frames = spectra.shape
    m = synth_taps.shape[1]
    own = frames // n
    chunks = own // W
    pieces = UP * own // DOWN // W
    wide = UP * m // DOWN // L
    blocks = m // L
    pin = lambda a: pltpu.with_memory_space_constraint(a, pltpu.HBM)
    vmem = pl.BlockSpec(memory_space=pltpu.VMEM)
    hbm = pl.BlockSpec(memory_space=pl.ANY)
    dma = pltpu.SemaphoreType.DMA
    out = pl.pallas_call(
        functools.partial(kernel, n),
        out_shape=jax.ShapeDtypeStruct((cb * 2 * UP * frames // DOWN // L, L), F32),
        in_specs=[hbm] * 5,
        out_specs=vmem,
        scratch_shapes=[
            pltpu.VMEM((cb * (2 * frames // L + 8), L), F32),
            pltpu.VMEM(synth_taps.shape, F32),
            pltpu.VMEM(analysis_taps.shape, F32),
            pltpu.VMEM((2, m, 2 * m), jnp.bfloat16),
            pltpu.VMEM((2, m + L, wide * L), jnp.bfloat16),
            pltpu.VMEM((n * chunks, cb, L), F32),
            pltpu.VMEM((chunks, n, cb, L), F32),
            pltpu.VMEM((chunks, 2, W, m), F32),
            pltpu.VMEM((2, HALO, m), F32),
            pltpu.VMEM((2, HALO + W, m), F32),
            pltpu.VMEM((2, 8 + BACK + W, m), F32),
            pltpu.VMEM((2, (BACK + W) * wide, L), F32),
            pltpu.VMEM((2, (BACK + own) * wide, L), F32),
            pltpu.VMEM((2, (BACK + W) * blocks, L), F32),
            pltpu.VMEM((2 * W, 2 * m), F32),
            pltpu.VMEM((pieces, n, cb, L), F32),
            pltpu.VMEM((pieces, n, cb, L), F32),
            dma((cb,)), dma, dma, dma, dma, dma((chunks,)), dma((chunks,)), dma, dma, dma((pieces,)), dma((pieces,)),
            pltpu.SemaphoreType.REGULAR((8,)),
        ],
        compiler_params=pltpu.CompilerParams(
            collective_id=0, has_side_effects=True, vmem_limit_bytes=40 << 20
        ),
    )(
        pin(rows_of(spectra)), pin(synth_taps), pin(analysis_taps),
        pin(halves(dft_table(m))), pin(halves(resample_table(m))),
    )
    return jnp.swapaxes(out.reshape(cb, -1, 2, L), 1, 2).reshape(cb, 2, -1)


def solution(mesh):
    in_specs = (P("tm", "station", None), P(), P())
    out_specs = P("tm", "station", None)
    body = functools.partial(shards, mesh.shape["tm"])
    return jax.shard_map(body, mesh=mesh, in_specs=in_specs, out_specs=out_specs, check_vma=False)
```

```python
import functools
import math

import jax
import jax.numpy as jnp
import numpy as np
from jax import lax
from jax.experimental import pallas as pl
from jax.experimental.pallas import tpu as pltpu
from jax.sharding import PartitionSpec as P

RT = 32
PHASES = 64
UP, DOWN = 5, 4
REACH = 8
W = 64
L = 128
HALO = 32
BACK = 16
MESH = pl.DeviceIdType.MESH
F32 = jnp.float32


def split(a):
    hi = a.astype(jnp.bfloat16)
    return hi, (a - hi.astype(F32)).astype(jnp.bfloat16)


def dft_table(width):
    k = np.outer(np.arange(width), np.arange(width)) % width
    angle = k * (2.0 * math.pi / width)
    both = np.concatenate([np.cos(angle), np.sin(angle)], axis=1) / math.sqrt(width)
    return both.astype(np.float32)


def resample_table(width):
    out_width = UP * width // DOWN
    sample = np.arange(out_width)[None, :]
    row = np.arange(L + width)[:, None]
    lag = DOWN * sample // UP + L - row
    phase = PHASES * (DOWN * sample % UP) // UP
    t = lag + phase / PHASES - (RT // 2 - 1)
    coeff = 0.9 * np.sinc(0.9 * t) * (0.5 + 0.5 * np.cos(math.pi * t / (RT / 2.0)))
    return np.where((lag >= 0) & (lag < RT), coeff, 0.0).astype(np.float32)


def halves(table):
    hi = table.astype(jnp.bfloat16)
    lo = (table - hi.astype(np.float32)).astype(jnp.bfloat16)
    return jnp.asarray(np.stack([hi, lo]))


def product(a, b, dims):
    (ah, al), (bh, bl) = a, b
    dot = lambda x, y: lax.dot_general(x, y, (dims, ((), ())), preferred_element_type=F32)
    return dot(ah, bh) + (dot(ah, bl) + dot(al, bh))


def kernel(
    n, x_hbm, st_hbm, at_hbm, cs_hbm, rs_hbm, o_ref,
    x_ref, st_ref, at_ref, cs, rs, xs, land1, v_all, hbuf, vwin, ywin, zst, zfull, zwin, u2, sbuf, land2,
    xsem, ssem, asem, csem, rsem, send1, recv1, hsend, hrecv, send2, recv2, ready,
):
    me = lax.axis_index("tm")
    station = lax.axis_index("station")
    nc = n // 2
    chip, core = me // 2, me % 2
    taps = st_ref.shape[0]
    m = st_ref.shape[1]
    chunks = land1.shape[0]
    pieces = land2.shape[0]
    cb = xs.shape[1]
    out_rows = o_ref.shape[0] // cb
    blocks = m // L

    def at(offset, c):
        return (chip + offset + nc) % nc * 2 + c

    def signal(sem, dev):
        pl.semaphore_signal(sem, inc=1, device_id=(station, dev), device_id_type=MESH)

    barrier = pltpu.get_barrier_semaphore()
    half = nc // 2
    reach = min(REACH, half)
    met = 1
    signal(barrier, at(0, 1 - core))
    for d in range(1, reach + 1):
        for offset in (d,) if 2 * d == nc else (d, -d):
            for c in range(2):
                signal(barrier, at(offset, c))
                met += 1
    in_rows = x_hbm.shape[0] // cb
    pitch = x_ref.shape[0] // cb
    get_x = [
        pltpu.make_async_copy(
            x_hbm.at[pl.ds(i * in_rows, in_rows)], x_ref.at[pl.ds(i * pitch, in_rows)], xsem.at[i]
        )
        for i in range(cb)
    ]
    for copy in get_x:
        copy.start()
    get_cs = pltpu.make_async_copy(cs_hbm, cs, csem)
    get_rs = pltpu.make_async_copy(rs_hbm, rs, rsem)
    get_st = pltpu.make_async_copy(st_hbm, st_ref, ssem)
    get_at = pltpu.make_async_copy(at_hbm, at_ref, asem)
    for copy in (get_cs, get_rs, get_st, get_at):
        copy.start()

    low = lax.broadcasted_iota(jnp.int32, (cb, L), 1) < W

    def arrange(i, c):
        for t in [chunks * i + j for j in range(chunks)]:
            a = x_ref[pl.ds(2 * t, cb, stride=pitch), :]
            b = x_ref[pl.ds(2 * t + 1, cb, stride=pitch), :]
            xs[2 * t] = jnp.where(low, a, pltpu.roll(b, W, 1))
            xs[2 * t + 1] = jnp.where(low, pltpu.roll(a, W, 1), b)
        return c

    def send_to(source, target, sent, got, near, far):
        def send(dev):
            pltpu.make_async_remote_copy(
                src_ref=source(dev), dst_ref=target, send_sem=sent, recv_sem=got,
                device_id=(station, dev), device_id_type=MESH,
            ).start()

        def step(j, c):
            d = far - j // 4
            sign = 1 - 2 * (j // 2 % 2)

            @pl.when(jnp.logical_not(jnp.logical_and(2 * d == nc, sign == -1)))
            def _():
                send(at(sign * d, (j + core) % 2))

            return c

        lax.fori_loop(0, 4 * (far - near + 1), step, 0)
        if near == 1:
            send(at(0, 1 - core))

    def send_in(k, near, far):
        send_to(lambda dev: xs.at[dev * chunks + k], land1.at[k, me], send1.at[k], recv1.at[k], near, far)

    def wait_bytes(ref, sem):
        part = ref.at[pl.ds(0, n - 1)]
        pltpu.make_async_copy(part, part, sem).wait()

    def synthesize(k):
        wait_bytes(land1.at[k], recv1.at[k])
        raw = land1[k].reshape(m, L)
        out = product(split(raw.T), (cs[0], cs[1]), ((1,), (0,)))
        v_all[k, 0] = out[:W, :m] - out[W:, m:]
        v_all[k, 1] = out[:W, m:] + out[W:, :m]

    last = chunks - 1
    for copy in get_x:
        copy.wait()
    lax.fori_loop(0, n // 2, arrange, 0)
    pl.semaphore_wait(barrier, met)
    known, turn, done = reach, 0, 0
    while known < half:
        for offset in (known, -known):
            signal(ready.at[turn], at(offset, core))
        for k in range(chunks):
            send_in((k - 1) % chunks, done + 1, known)
        done = known
        pl.semaphore_wait(ready.at[turn], 2)
        known, turn = min(2 * known, half), turn + 1
    send_in(last, done + 1, half)
    send_in(0, done + 1, half)
    for k in range(chunks):
        land1[k, me] = xs[me * chunks + k]
    ywin[:, 0:8, :] = jnp.zeros((2, 8, m), F32)
    get_cs.wait()
    synthesize(last)
    tail = pltpu.make_async_remote_copy(
        src_ref=v_all.at[last, :, pl.ds(W - HALO, HALO)], dst_ref=hbuf,
        send_sem=hsend, recv_sem=hrecv,
        device_id=(station, (me + 1) % n), device_id_type=MESH,
    )

    @pl.when(me < n - 1)
    def _():
        tail.start()

    for k in range(1, last):
        send_in(k, done + 1, half)
    for copy in (get_rs, get_st, get_at):
        copy.wait()

    def resampled(k):
        @pl.when(k == 0)
        def _():
            @pl.when(me == 0)
            def _():
                vwin[:, 0:HALO, :] = jnp.zeros((2, HALO, m), F32)

            @pl.when(me > 0)
            def _():
                tail.wait_recv()
                vwin[:, 0:HALO, :] = hbuf[...]

        @pl.when(k > 0)
        def _():
            vwin[:, 0:HALO, :] = vwin[:, W : W + HALO, :]

        vwin[:, HALO:, :] = v_all[k]
        rows = BACK + W
        for ri in range(2):
            for b in range(blocks):
                lanes = pl.ds(b * L, L)
                total = jnp.zeros((rows, L), F32)
                for p in range(taps):
                    total = total + st_ref[p : p + 1, lanes] * vwin[ri, pl.ds(BACK - p, rows), lanes]
                ywin[ri, pl.ds(8, rows), lanes] = total
        left = jnp.concatenate(
            [
                jnp.concatenate([ywin[ri, pl.ds(7, rows), pl.ds(m - L, L)], ywin[ri, pl.ds(8, rows), :]], axis=1)
                for ri in range(2)
            ],
            axis=0,
        )
        out = product(split(left), (rs[0], rs[1]), ((1,), (0,)))
        wide = UP * blocks // DOWN
        for ri in range(2):
            for j in range(wide):
                zst[ri, pl.ds(j, rows, stride=wide), :] = out[ri * rows : (ri + 1) * rows, j * L : (j + 1) * L]

        @pl.when(k == 0)
        def _():
            zfull[:, 0 : BACK * wide, :] = zst[:, 0 : BACK * wide, :]

        zfull[:, pl.ds(pl.multiple_of(BACK * wide + k * (W * wide), 8), W * wide), :] = zst[:, BACK * wide :, :]

    def analyzed(p):
        wide = UP * blocks // DOWN
        first = BACK * wide - BACK * blocks
        zwin[...] = zfull[:, pl.ds(pl.multiple_of(first + p * (W * blocks), 8), (BACK + W) * blocks), :]
        for b in range(blocks):
            for ri in range(2):
                total = jnp.zeros((W, L), F32)
                for t in range(taps):
                    total = total + at_ref[t : t + 1, pl.ds(b * L, L)] * zwin[
                        ri, pl.ds((BACK - t) * blocks + b, W, stride=blocks), :
                    ]
                if ri == 0:
                    u2[0:W, pl.ds(b * L, L)] = total
                    u2[W:, pl.ds(m + b * L, L)] = -total
                else:
                    u2[0:W, pl.ds(m + b * L, L)] = total
                    u2[W:, pl.ds(b * L, L)] = total
        out = product((cs[0], cs[1]), split(u2[...]), ((1,), (1,)))
        sbuf[p] = out.reshape(n, cb, L)
        land2[p, me] = sbuf[p, me]
        send_to(lambda dev: sbuf.at[p, dev], land2.at[p, me], send2.at[p], recv2.at[p], 1, nc // 2)

    def step(p, c):
        @pl.when(p < last)
        def _():
            synthesize(p)

        @pl.when(p < chunks)
        def _():
            resampled(p)

        analyzed(p)
        return c

    lax.fori_loop(0, pieces, step, 0)

    @pl.when(me < n - 1)
    def _():
        tail.wait_send()

    for k in range(chunks):
        wait_bytes(land1.at[k], send1.at[k])
    for p in range(pieces):
        wait_bytes(land2.at[p], recv2.at[p])
        pairs = [(u, divmod(2 * u, pieces), divmod(2 * u + 1, pieces)) for u in range(pieces)]
        pairs = [pair for pair in pairs if max(pair[1][1], pair[2][1]) == p]

        def place(t, c, pairs=pairs):
            for u, (da, pa), (db, pb) in pairs:
                a = land2[pa, 2 * t + da]
                b = land2[pb, 2 * t + db]
                first = 2 * (t * pieces + u)
                o_ref[pl.ds(first, cb, stride=out_rows), :] = jnp.where(low, a, pltpu.roll(b, W, 1))
                o_ref[pl.ds(first + 1, cb, stride=out_rows), :] = jnp.where(low, pltpu.roll(a, W, 1), b)
            return c

        if pairs:
            lax.fori_loop(0, n // 2, place, 0)

    for p in range(pieces):
        wait_bytes(land2.at[p], send2.at[p])


def rows_of(spectra):
    parts = spectra.reshape(spectra.shape[0], 2, -1, L)
    return jnp.swapaxes(parts, 1, 2).reshape(-1, L)


def shards(n, spectra, synth_taps, analysis_taps):
    cb, _, frames = spectra.shape
    m = synth_taps.shape[1]
    own = frames // n
    chunks = own // W
    pieces = UP * own // DOWN // W
    wide = UP * m // DOWN // L
    blocks = m // L
    pin = lambda a: pltpu.with_memory_space_constraint(a, pltpu.HBM)
    vmem = pl.BlockSpec(memory_space=pltpu.VMEM)
    hbm = pl.BlockSpec(memory_space=pl.ANY)
    dma = pltpu.SemaphoreType.DMA
    out = pl.pallas_call(
        functools.partial(kernel, n),
        out_shape=jax.ShapeDtypeStruct((cb * 2 * UP * frames // DOWN // L, L), F32),
        in_specs=[hbm] * 5,
        out_specs=vmem,
        scratch_shapes=[
            pltpu.VMEM((cb * (2 * frames // L + 8), L), F32),
            pltpu.VMEM(synth_taps.shape, F32),
            pltpu.VMEM(analysis_taps.shape, F32),
            pltpu.VMEM((2, m, 2 * m), jnp.bfloat16),
            pltpu.VMEM((2, m + L, wide * L), jnp.bfloat16),
            pltpu.VMEM((n * chunks, cb, L), F32),
            pltpu.VMEM((chunks, n, cb, L), F32),
            pltpu.VMEM((chunks, 2, W, m), F32),
            pltpu.VMEM((2, HALO, m), F32),
            pltpu.VMEM((2, HALO + W, m), F32),
            pltpu.VMEM((2, 8 + BACK + W, m), F32),
            pltpu.VMEM((2, (BACK + W) * wide, L), F32),
            pltpu.VMEM((2, (BACK + own) * wide, L), F32),
            pltpu.VMEM((2, (BACK + W) * blocks, L), F32),
            pltpu.VMEM((2 * W, 2 * m), F32),
            pltpu.VMEM((pieces, n, cb, L), F32),
            pltpu.VMEM((pieces, n, cb, L), F32),
            dma((cb,)), dma, dma, dma, dma, dma((chunks,)), dma((chunks,)), dma, dma, dma((pieces,)), dma((pieces,)),
            pltpu.SemaphoreType.REGULAR((8,)),
        ],
        compiler_params=pltpu.CompilerParams(
            collective_id=0, has_side_effects=True, vmem_limit_bytes=40 << 20
        ),
    )(
        pin(rows_of(spectra)), pin(synth_taps), pin(analysis_taps),
        pin(halves(dft_table(m))), pin(halves(resample_table(m))),
    )
    return jnp.swapaxes(out.reshape(cb, -1, 2, L), 1, 2).reshape(cb, 2, -1)


def solution(mesh):
    in_specs = (P("tm", "station", None), P(), P())
    out_specs = P("tm", "station", None)
    body = functools.partial(shards, mesh.shape["tm"])
    return jax.shard_map(body, mesh=mesh, in_specs=in_specs, out_specs=out_specs, check_vma=False)
```

```python
import functools
import math

import jax
import jax.numpy as jnp
import numpy as np
from jax import lax
from jax.experimental import pallas as pl
from jax.experimental.pallas import tpu as pltpu
from jax.sharding import PartitionSpec as P

RT = 32
PHASES = 64
UP, DOWN = 5, 4
REACH = 8
W = 64
L = 128
HALO = 32
BACK = 16
MESH = pl.DeviceIdType.MESH
F32 = jnp.float32


def split(a):
    hi = a.astype(jnp.bfloat16)
    return hi, (a - hi.astype(F32)).astype(jnp.bfloat16)


def dft_table(width):
    k = np.outer(np.arange(width), np.arange(width)) % width
    angle = k * (2.0 * math.pi / width)
    both = np.concatenate([np.cos(angle), np.sin(angle)], axis=1) / math.sqrt(width)
    return both.astype(np.float32)


def resample_table(width):
    out_width = UP * width // DOWN
    sample = np.arange(out_width)[None, :]
    row = np.arange(L + width)[:, None]
    lag = DOWN * sample // UP + L - row
    phase = PHASES * (DOWN * sample % UP) // UP
    t = lag + phase / PHASES - (RT // 2 - 1)
    coeff = 0.9 * np.sinc(0.9 * t) * (0.5 + 0.5 * np.cos(math.pi * t / (RT / 2.0)))
    return np.where((lag >= 0) & (lag < RT), coeff, 0.0).astype(np.float32)


def halves(table):
    hi = table.astype(jnp.bfloat16)
    lo = (table - hi.astype(np.float32)).astype(jnp.bfloat16)
    return jnp.asarray(np.stack([hi, lo]))


def product(a, b, dims):
    (ah, al), (bh, bl) = a, b
    dot = lambda x, y: lax.dot_general(x, y, (dims, ((), ())), preferred_element_type=F32)
    return dot(ah, bh) + (dot(ah, bl) + dot(al, bh))


def kernel(
    n, x_hbm, st_hbm, at_hbm, cs_hbm, rs_hbm, o_ref,
    x_ref, st_ref, at_ref, cs, rs, xs, land1, v_all, hbuf, vwin, ywin, zst, zfull, zwin, u2, sbuf, land2,
    xsem, ssem, asem, csem, rsem, send1, recv1, hsend, hrecv, send2, recv2, ready,
):
    me = lax.axis_index("tm")
    station = lax.axis_index("station")
    nc = n // 2
    chip, core = me // 2, me % 2
    taps = st_ref.shape[0]
    m = st_ref.shape[1]
    chunks = land1.shape[0]
    pieces = land2.shape[0]
    cb = xs.shape[1]
    out_rows = o_ref.shape[0] // cb
    blocks = m // L

    def at(offset, c):
        return (chip + offset + nc) % nc * 2 + c

    def signal(sem, dev):
        pl.semaphore_signal(sem, inc=1, device_id=(station, dev), device_id_type=MESH)

    barrier = pltpu.get_barrier_semaphore()
    half = nc // 2
    reach = min(REACH, half)
    met = 1
    signal(barrier, at(0, 1 - core))
    for d in range(1, reach + 1):
        for offset in (d,) if 2 * d == nc else (d, -d):
            for c in range(2):
                signal(barrier, at(offset, c))
                met += 1
    in_rows = x_hbm.shape[0] // cb
    pitch = x_ref.shape[0] // cb
    get_x = [
        pltpu.make_async_copy(
            x_hbm.at[pl.ds(i * in_rows, in_rows)], x_ref.at[pl.ds(i * pitch, in_rows)], xsem.at[i]
        )
        for i in range(cb)
    ]
    for copy in get_x:
        copy.start()
    get_cs = pltpu.make_async_copy(cs_hbm, cs, csem)
    get_rs = pltpu.make_async_copy(rs_hbm, rs, rsem)
    get_st = pltpu.make_async_copy(st_hbm, st_ref, ssem)
    get_at = pltpu.make_async_copy(at_hbm, at_ref, asem)
    for copy in (get_cs, get_rs, get_st, get_at):
        copy.start()

    low = lax.broadcasted_iota(jnp.int32, (cb, L), 1) < W

    def arrange(i, c):
        for t in [chunks * i + j for j in range(chunks)]:
            a = x_ref[pl.ds(2 * t, cb, stride=pitch), :]
            b = x_ref[pl.ds(2 * t + 1, cb, stride=pitch), :]
            xs[2 * t] = jnp.where(low, a, pltpu.roll(b, W, 1))
            xs[2 * t + 1] = jnp.where(low, pltpu.roll(a, W, 1), b)
        return c

    def send_to(source, target, sent, got, near, far):
        def send(dev):
            pltpu.make_async_remote_copy(
                src_ref=source(dev), dst_ref=target, send_sem=sent, recv_sem=got,
                device_id=(station, dev), device_id_type=MESH,
            ).start()

        def step(j, c):
            d = far - j // 4
            sign = 1 - 2 * ((j // 2 + core) % 2)

            @pl.when(jnp.logical_not(jnp.logical_and(2 * d == nc, sign == -1)))
            def _():
                send(at(sign * d, (j + core) % 2))

            return c

        lax.fori_loop(0, 4 * (far - near + 1), step, 0)
        if near == 1:
            send(at(0, 1 - core))

    def send_in(k, near, far):
        send_to(lambda dev: xs.at[dev * chunks + k], land1.at[k, me], send1.at[k], recv1.at[k], near, far)

    def wait_bytes(ref, sem):
        part = ref.at[pl.ds(0, n - 1)]
        pltpu.make_async_copy(part, part, sem).wait()

    def synthesize(k):
        wait_bytes(land1.at[k], recv1.at[k])
        raw = land1[k].reshape(m, L)
        out = product(split(raw.T), (cs[0], cs[1]), ((1,), (0,)))
        v_all[k, 0] = out[:W, :m] - out[W:, m:]
        v_all[k, 1] = out[:W, m:] + out[W:, :m]

    last = chunks - 1
    for copy in get_x:
        copy.wait()
    lax.fori_loop(0, n // 2, arrange, 0)
    pl.semaphore_wait(barrier, met)
    known, turn = reach, 0
    done = [0] * chunks
    while known < half:
        for offset in (known, -known):
            signal(ready.at[turn], at(offset, core))
        for k in (last, *range(last)):
            if 2 * known < half or k in (last, 0):
                send_in(k, done[k] + 1, known)
                done[k] = known
        pl.semaphore_wait(ready.at[turn], 2)
        known, turn = min(2 * known, half), turn + 1
    send_in(last, done[last] + 1, half)
    send_in(0, done[0] + 1, half)
    for k in range(chunks):
        land1[k, me] = xs[me * chunks + k]
    ywin[:, 0:8, :] = jnp.zeros((2, 8, m), F32)
    get_cs.wait()
    synthesize(last)
    tail = pltpu.make_async_remote_copy(
        src_ref=v_all.at[last, :, pl.ds(W - HALO, HALO)], dst_ref=hbuf,
        send_sem=hsend, recv_sem=hrecv,
        device_id=(station, (me + 1) % n), device_id_type=MESH,
    )

    @pl.when(me < n - 1)
    def _():
        tail.start()

    for k in range(1, last):
        send_in(k, done[k] + 1, half)
    for copy in (get_rs, get_st, get_at):
        copy.wait()

    def resampled(k):
        @pl.when(k == 0)
        def _():
            @pl.when(me == 0)
            def _():
                vwin[:, 0:HALO, :] = jnp.zeros((2, HALO, m), F32)

            @pl.when(me > 0)
            def _():
                tail.wait_recv()
                vwin[:, 0:HALO, :] = hbuf[...]

        @pl.when(k > 0)
        def _():
            vwin[:, 0:HALO, :] = vwin[:, W : W + HALO, :]

        vwin[:, HALO:, :] = v_all[k]
        rows = BACK + W
        for ri in range(2):
            for b in range(blocks):
                lanes = pl.ds(b * L, L)
                total = jnp.zeros((rows, L), F32)
                for p in range(taps):
                    total = total + st_ref[p : p + 1, lanes] * vwin[ri, pl.ds(BACK - p, rows), lanes]
                ywin[ri, pl.ds(8, rows), lanes] = total
        left = jnp.concatenate(
            [
                jnp.concatenate([ywin[ri, pl.ds(7, rows), pl.ds(m - L, L)], ywin[ri, pl.ds(8, rows), :]], axis=1)
                for ri in range(2)
            ],
            axis=0,
        )
        out = product(split(left), (rs[0], rs[1]), ((1,), (0,)))
        wide = UP * blocks // DOWN
        for ri in range(2):
            for j in range(wide):
                zst[ri, pl.ds(j, rows, stride=wide), :] = out[ri * rows : (ri + 1) * rows, j * L : (j + 1) * L]

        @pl.when(k == 0)
        def _():
            zfull[:, 0 : BACK * wide, :] = zst[:, 0 : BACK * wide, :]

        zfull[:, pl.ds(pl.multiple_of(BACK * wide + k * (W * wide), 8), W * wide), :] = zst[:, BACK * wide :, :]

    def analyzed(p):
        wide = UP * blocks // DOWN
        first = BACK * wide - BACK * blocks
        zwin[...] = zfull[:, pl.ds(pl.multiple_of(first + p * (W * blocks), 8), (BACK + W) * blocks), :]
        for b in range(blocks):
            for ri in range(2):
                total = jnp.zeros((W, L), F32)
                for t in range(taps):
                    total = total + at_ref[t : t + 1, pl.ds(b * L, L)] * zwin[
                        ri, pl.ds((BACK - t) * blocks + b, W, stride=blocks), :
                    ]
                if ri == 0:
                    u2[0:W, pl.ds(b * L, L)] = total
                    u2[W:, pl.ds(m + b * L, L)] = -total
                else:
                    u2[0:W, pl.ds(m + b * L, L)] = total
                    u2[W:, pl.ds(b * L, L)] = total
        out = product((cs[0], cs[1]), split(u2[...]), ((1,), (1,)))
        sbuf[p] = out.reshape(n, cb, L)
        land2[p, me] = sbuf[p, me]
        send_to(lambda dev: sbuf.at[p, dev], land2.at[p, me], send2.at[p], recv2.at[p], 1, nc // 2)

    def step(p, c):
        @pl.when(p < last)
        def _():
            synthesize(p)

        @pl.when(p < chunks)
        def _():
            resampled(p)

        analyzed(p)
        return c

    lax.fori_loop(0, pieces, step, 0)

    @pl.when(me < n - 1)
    def _():
        tail.wait_send()

    for k in range(chunks):
        wait_bytes(land1.at[k], send1.at[k])
    for p in range(pieces):
        wait_bytes(land2.at[p], recv2.at[p])
        pairs = [(u, divmod(2 * u, pieces), divmod(2 * u + 1, pieces)) for u in range(pieces)]
        pairs = [pair for pair in pairs if max(pair[1][1], pair[2][1]) == p]

        def place(t, c, pairs=pairs):
            for u, (da, pa), (db, pb) in pairs:
                a = land2[pa, 2 * t + da]
                b = land2[pb, 2 * t + db]
                first = 2 * (t * pieces + u)
                o_ref[pl.ds(first, cb, stride=out_rows), :] = jnp.where(low, a, pltpu.roll(b, W, 1))
                o_ref[pl.ds(first + 1, cb, stride=out_rows), :] = jnp.where(low, pltpu.roll(a, W, 1), b)
            return c

        if pairs:
            lax.fori_loop(0, n // 2, place, 0)

    for p in range(pieces):
        wait_bytes(land2.at[p], send2.at[p])


def rows_of(spectra):
    parts = spectra.reshape(spectra.shape[0], 2, -1, L)
    return jnp.swapaxes(parts, 1, 2).reshape(-1, L)


def shards(n, spectra, synth_taps, analysis_taps):
    cb, _, frames = spectra.shape
    m = synth_taps.shape[1]
    own = frames // n
    chunks = own // W
    pieces = UP * own // DOWN // W
    wide = UP * m // DOWN // L
    blocks = m // L
    pin = lambda a: pltpu.with_memory_space_constraint(a, pltpu.HBM)
    vmem = pl.BlockSpec(memory_space=pltpu.VMEM)
    hbm = pl.BlockSpec(memory_space=pl.ANY)
    dma = pltpu.SemaphoreType.DMA
    out = pl.pallas_call(
        functools.partial(kernel, n),
        out_shape=jax.ShapeDtypeStruct((cb * 2 * UP * frames // DOWN // L, L), F32),
        in_specs=[hbm] * 5,
        out_specs=vmem,
        scratch_shapes=[
            pltpu.VMEM((cb * (2 * frames // L + 8), L), F32),
            pltpu.VMEM(synth_taps.shape, F32),
            pltpu.VMEM(analysis_taps.shape, F32),
            pltpu.VMEM((2, m, 2 * m), jnp.bfloat16),
            pltpu.VMEM((2, m + L, wide * L), jnp.bfloat16),
            pltpu.VMEM((n * chunks, cb, L), F32),
            pltpu.VMEM((chunks, n, cb, L), F32),
            pltpu.VMEM((chunks, 2, W, m), F32),
            pltpu.VMEM((2, HALO, m), F32),
            pltpu.VMEM((2, HALO + W, m), F32),
            pltpu.VMEM((2, 8 + BACK + W, m), F32),
            pltpu.VMEM((2, (BACK + W) * wide, L), F32),
            pltpu.VMEM((2, (BACK + own) * wide, L), F32),
            pltpu.VMEM((2, (BACK + W) * blocks, L), F32),
            pltpu.VMEM((2 * W, 2 * m), F32),
            pltpu.VMEM((pieces, n, cb, L), F32),
            pltpu.VMEM((pieces, n, cb, L), F32),
            dma((cb,)), dma, dma, dma, dma, dma((chunks,)), dma((chunks,)), dma, dma, dma((pieces,)), dma((pieces,)),
            pltpu.SemaphoreType.REGULAR((8,)),
        ],
        compiler_params=pltpu.CompilerParams(
            collective_id=0, has_side_effects=True, vmem_limit_bytes=40 << 20
        ),
    )(
        pin(rows_of(spectra)), pin(synth_taps), pin(analysis_taps),
        pin(halves(dft_table(m))), pin(halves(resample_table(m))),
    )
    return jnp.swapaxes(out.reshape(cb, -1, 2, L), 1, 2).reshape(cb, 2, -1)


def solution(mesh):
    in_specs = (P("tm", "station", None), P(), P())
    out_specs = P("tm", "station", None)
    body = functools.partial(shards, mesh.shape["tm"])
    return jax.shard_map(body, mesh=mesh, in_specs=in_specs, out_specs=out_specs, check_vma=False)
```
